32 devices in a mesh: group: 2 (over y), cp: 8 (over z, x), hd: 2 (over core).
Axes of the slice: x: 2, y: 2, z: 4, core: 2. Of those that a mesh axis runs over, the one named last changes fastest.
Arguments:
- doc_lengths: int32 [8], P('group'), parts along dimension 0, may hold values from 1 to 384, 1024 in all
- queries: bfloat16 [2048, 4096], P(('group', 'cp'), 'hd'), parts along dimension 0, may hold values from -52 to 52
- key_states: bfloat16 [2048, 1024], P(('group', 'cp'), 'hd'), parts along dimension 0, may hold values from -4 to 4
- value_head_states: bfloat16 [2048, 1024], P(('group', 'cp'), 'hd'), parts along dimension 0, may hold values from -6 to 6
- out_grad: bfloat16 [2048, 4096], P(('group', 'cp'), 'hd'), parts along dimension 0, may hold values from -6 to 6
Outputs:
- attended: bfloat16 [2048, 4096], P(('group', 'cp'), 'hd'), parts along dimension 0
- grad_queries: bfloat16 [2048, 4096], P(('group', 'cp'), 'hd'), parts along dimension 0
- grad_keys: bfloat16 [2048, 1024], P(('group', 'cp'), 'hd'), parts along dimension 0
- grad_values: bfloat16 [2048, 1024], P(('group', 'cp'), 'hd'), parts along dimension 0
The draws below stay inside these ranges and needn't reach their ends.
There are 2 independent parts, one for each index of `group`. The reference program is written for one: setup_inputs(seed, part) draws one part's arguments, and reference() takes and returns one part's arrays. A program takes and returns all parts, laid end to end along the dimension named above; each array names one. Nothing has to cross between parts.
Inputs may be any that keep to these rules, and one draw needn't show every extreme that they name: `doc_lengths`: documents lie end to end in token order; their lengths sum to 1024.
All inputs are finite; a program needn't handle non-finite values.
Results may differ from the reference program's by a relative error of at most 0.028.
Values may be sent and summed in bfloat16 or wider, within the bound.
A program may use at most 64 MiB of HBM per device.

```python
import math
import jax
import jax.numpy as jnp
import numpy as np
from jax import lax

QUERY_HEADS_COUNT = 32
KEY_VALUE_HEADS = 8
HEAD_SIZE = 128
TOK_DEV = 128
REACH = 3
WINDOW_TOKENS = 1024
MAXDOC = 384
DOCS = 4
N_CP = 8


def starting_keys(key):
    array_extent = (WINDOW_TOKENS, KEY_VALUE_HEADS * HEAD_SIZE)
    sampled_values = jax.random.truncated_normal(jax.random.fold_in(key, 12), -4.0, 4.0, array_extent, jnp.float32)
    return sampled_values


def draw_key_states(key, part):
    sampled_values = starting_keys(key)
    return sampled_values.astype(jnp.bfloat16)


def draw_queries(key, part):
    array_extent = (WINDOW_TOKENS, QUERY_HEADS_COUNT * HEAD_SIZE)
    sampled_values = jax.random.truncated_normal(jax.random.fold_in(key, 13), -4.0, 4.0, array_extent, jnp.float32)
    return sampled_values.astype(jnp.bfloat16)


def level_of(stream_key, shape, pieces, smallest, high):
    factor_of, own = 1.0, jax.random.fold_in(stream_key, 6)
    for dim, shards_of in pieces:
        draws = jnp.exp(jax.random.uniform(jax.random.fold_in(own, dim), (shards_of,), jnp.float32, smallest / len(pieces), high / len(pieces)))
        factor_of = factor_of * jnp.repeat(draws, shape[dim] // shards_of).reshape([-1 if axis == dim else 1 for axis in range(len(shape))])
    return factor_of


def length_profile(count, total, bound, slope):
    loads = [(1 << 20) // math.isqrt(grade ** slope) + 1 for grade in range(2, count + 1)]
    rest, given = total - bound - (count - 1), [1] * (count - 1)
    while rest > 0:
        candidates = [i for i in range(count - 1) if given[i] < bound]
        pool, budget = sum([loads[i] for i in candidates]), rest
        for i in candidates:
            extra = min(bound - given[i], max(1, budget * loads[i] // pool), rest)
            given[i] = given[i] + extra
            rest = rest - extra
    return np.array([bound] + given)


def uneven_parts(own_key, amount, total, limit, skew):
    if amount == 2:
        one = jax.random.randint(own_key, (), max(1, total - limit), min(limit, total - 1) + 1)
        return jnp.stack([one, total - one])
    lengths = jnp.asarray(length_profile(amount, total, limit, skew), jnp.int32)
    twos = (amount - 1) // 2
    giver, receiver = lengths[1:1 + 2 * twos:2], lengths[2:2 + 2 * twos:2]
    margin = jnp.minimum(giver - 1, limit - receiver)
    passed = jax.random.randint(jax.random.fold_in(own_key, 1), (twos,), 0, 1 << 20) % (margin + 1)
    lengths = lengths.at[1:1 + 2 * twos:2].set(giver - passed).at[2:2 + 2 * twos:2].set(receiver + passed)
    return lengths[jax.random.permutation(jax.random.fold_in(own_key, 2), amount)]


def scatter_about(rng, dims, scale, bound, pieces=(), kind=jnp.bfloat16):
    values = jax.random.normal(rng, dims, jnp.float32) * scale
    if len(pieces) > 0:
        values = level_of(rng, dims, pieces, -0.22, 0.18) * values
    return jnp.clip(values, min=-bound, max=bound).astype(kind)


def setup_inputs(seed: int = 0, part: int = 0) -> dict:
    arg_keys = jax.random.split(jax.random.key(seed), 6)
    own_keys = jax.random.split(jax.random.fold_in(arg_keys[5], part), 6)
    return {
        "doc_lengths": uneven_parts(own_keys[0], DOCS, WINDOW_TOKENS, MAXDOC, 2).astype(jnp.int32),
        "queries": draw_queries(jax.random.fold_in(jax.random.fold_in(arg_keys[5], part), 71), part),
        "key_states": draw_key_states(jax.random.fold_in(jax.random.fold_in(arg_keys[5], part), 71), part),
        "value_head_states": scatter_about(own_keys[3], (WINDOW_TOKENS, KEY_VALUE_HEADS * HEAD_SIZE), 1.0, 6.0, ((0, 8), (1, 2))),
        "out_grad": scatter_about(own_keys[4], (WINDOW_TOKENS, QUERY_HEADS_COUNT * HEAD_SIZE), 1.0, 6.0, ((0, 8), (1, 2))),
    }


masked_score = -1e+30

def document_ids(doc_lengths, positions):
    ends = jnp.cumsum(doc_lengths).astype(jnp.int32)
    counted = lax.optimization_barrier(jnp.sum((ends[None, :] <= positions[:, None]).astype(jnp.int32), axis=1)).astype(jnp.int32)
    return jnp.where(positions < 0, jnp.int32(-1), counted)

def attend(queries, key_rows, value_rows, out_grad, allowed):
    tok_rows = queries.shape[0]
    window_rows = key_rows.shape[0]
    head_kv = key_rows.shape[1] // HEAD_SIZE
    group_size = queries.shape[1] // key_rows.shape[1]
    score_scale = 1.0 / math.sqrt(HEAD_SIZE)
    query_heads = queries.reshape(tok_rows, head_kv, group_size, HEAD_SIZE).astype(jnp.float32)
    key_heads = key_rows.reshape(window_rows, head_kv, HEAD_SIZE).astype(jnp.float32)
    value_heads = value_rows.reshape(window_rows, head_kv, HEAD_SIZE).astype(jnp.float32)
    grad_heads = out_grad.reshape(tok_rows, head_kv, group_size, HEAD_SIZE).astype(jnp.float32)
    scores = jnp.einsum('qhgd,khd->hgqk', query_heads, key_heads) * score_scale
    scores = jnp.where(allowed, scores, masked_score)
    row_max = lax.optimization_barrier(jnp.max(scores, axis=-1, keepdims=True))
    weights_raw = jnp.exp(scores - row_max)
    probs = weights_raw / lax.optimization_barrier(jnp.sum(weights_raw, axis=-1, keepdims=True))
    probs_low = probs.astype(jnp.bfloat16).astype(jnp.float32)
    attended = jnp.einsum('hgqk,khd->qhgd', probs_low, value_heads).astype(jnp.bfloat16)
    delta = lax.optimization_barrier(jnp.sum(grad_heads * attended.astype(jnp.float32), axis=-1)).transpose(1, 2, 0)
    grad_value = jnp.einsum('hgqk,qhgd->khd', probs_low, grad_heads)
    grad_probs = jnp.einsum('qhgd,khd->hgqk', grad_heads, value_heads)
    grad_scores = (probs * (grad_probs - delta[..., None])).astype(jnp.bfloat16).astype(jnp.float32)
    grad_query = (jnp.einsum('hgqk,khd->qhgd', grad_scores, key_heads) * score_scale).astype(jnp.bfloat16)
    grad_key = jnp.einsum('hgqk,qhgd->khd', grad_scores, query_heads) * score_scale
    return (attended.reshape(tok_rows, -1), grad_query.reshape(tok_rows, -1), grad_key.reshape(window_rows, -1), grad_value.reshape(window_rows, -1))

def reference(doc_lengths, queries, key_states, value_head_states, out_grad):
    tok_rows = TOK_DEV
    window_rows = (REACH + 1) * tok_rows
    pad_rows = REACH * tok_rows
    columns = key_states.shape[1]
    padding = jnp.zeros((pad_rows, columns), key_states.dtype)
    keys_padded = jnp.concatenate([padding, key_states], axis=0)
    values_padded = jnp.concatenate([padding, value_head_states], axis=0)
    empty = jnp.zeros((pad_rows + WINDOW_TOKENS, columns), jnp.float32)

    def block_step(carry, block_index):
        sum_keys, sum_values = carry
        row_start = (block_index * tok_rows).astype(jnp.int32)
        query_block = lax.dynamic_slice_in_dim(queries, row_start, tok_rows, 0)
        grad_block = lax.dynamic_slice_in_dim(out_grad, row_start, tok_rows, 0)
        key_block = lax.dynamic_slice_in_dim(keys_padded, row_start, window_rows, 0)
        value_block = lax.dynamic_slice_in_dim(values_padded, row_start, window_rows, 0)
        query_pos = row_start + lax.iota(jnp.int32, tok_rows)
        key_pos = row_start - pad_rows + lax.iota(jnp.int32, window_rows)
        query_ids = document_ids(doc_lengths, query_pos)
        key_ids = document_ids(doc_lengths, key_pos)
        allowed = (query_ids[:, None] == key_ids[None, :]) & (key_pos[None, :] <= query_pos[:, None])
        attended, grad_query, grad_key, grad_value = attend(query_block, key_block, value_block, grad_block, allowed)
        old_keys = lax.dynamic_slice_in_dim(sum_keys, row_start, window_rows, 0)
        old_values = lax.dynamic_slice_in_dim(sum_values, row_start, window_rows, 0)
        sum_keys = lax.dynamic_update_slice_in_dim(sum_keys, old_keys + grad_key, row_start, 0)
        sum_values = lax.dynamic_update_slice_in_dim(sum_values, old_values + grad_value, row_start, 0)
        return ((sum_keys, sum_values), (attended, grad_query))
    (sum_keys, sum_values), (outs, grads) = lax.scan(block_step, (empty, empty), jnp.arange(N_CP, dtype=jnp.int32))
    attended = outs.reshape(WINDOW_TOKENS, -1)
    grad_queries = grads.reshape(WINDOW_TOKENS, -1)
    grad_keys = sum_keys[pad_rows:].astype(jnp.bfloat16)
    grad_values = sum_values[pad_rows:].astype(jnp.bfloat16)
    return (attended, grad_queries, grad_keys, grad_values)
```

```python
import functools
import math

import jax
import jax.numpy as jnp
from jax import lax
from jax.experimental import pallas as pl
from jax.experimental.pallas import tpu as pltpu
from jax.sharding import PartitionSpec as P

HEAD = 128
REACH = 3
MASKED = -1e30
MESH = pl.DeviceIdType.MESH
X, B, T = range(3)


def kernel(
    n, docs, doc_hbm, q_hbm, k_hbm, v_hbm, do_hbm, o_ref, gq_ref, gk_ref, gv_ref,
    kv, qb, db, own, mid, part, back, bias, doc_ref,
    doc_sem, kv_sem, q_sem, fs_sem, fr_sem, bs_sem, br_sem,
):
    tok = q_hbm.shape[0]
    heads = k_hbm.shape[1] // HEAD
    group = q_hbm.shape[1] // k_hbm.shape[1]
    me = lax.axis_index("cp")
    odd = lax.rem(me, 2)
    is_odd = odd == 1
    is_even = odd == 0
    partner = me + 1 - 2 * odd
    own_rows = pl.ds(REACH * tok, tok)

    def rows(dist):
        return pl.ds((REACH - dist) * tok, tok)

    def cols(h):
        return pl.ds(h * HEAD, HEAD)

    doc_load = pltpu.make_async_copy(doc_hbm, doc_ref, doc_sem)
    doc_load.start()
    kv_loads = []
    for g in range(heads):
        kv_loads.append([
            pltpu.make_async_copy(src.at[:, cols(g)], kv.at[g, t, own_rows], kv_sem.at[g, t])
            for t, src in enumerate((k_hbm, v_hbm))
        ])
        for c in kv_loads[g]:
            c.start()
    q_loads = []
    for h in range(heads * group):
        q_loads.append([
            pltpu.make_async_copy(q_hbm.at[:, cols(h)], qb.at[h], q_sem.at[0, h]),
            pltpu.make_async_copy(do_hbm.at[:, cols(h)], db.at[h], q_sem.at[1, h]),
        ])
        for c in q_loads[h]:
            c.start()

    barrier = pltpu.get_barrier_semaphore()
    for to, cond in ((me - 2, me >= 2), (me + 2, me + 2 < n), (partner, me >= 0)):
        @pl.when(cond)
        def _():
            pl.semaphore_signal(barrier, inc=1, device_id={"cp": to}, device_id_type=MESH)
    pl.semaphore_wait(
        barrier, 1 + jnp.minimum(me // 2, 1) + jnp.minimum((n - 1 - me) // 2, 1))

    def fwd(kind, g, src_rows, dst_rows, to):
        return pltpu.make_async_remote_copy(
            src_ref=kv.at[g, :, src_rows], dst_ref=kv.at[g, :, dst_rows],
            send_sem=fs_sem.at[kind, g], recv_sem=fr_sem.at[kind, g],
            device_id={"cp": to}, device_id_type=MESH,
        )

    def fwd_x(g):
        return fwd(X, g, pl.ds((REACH - 2 * odd) * tok, tok), rows(1), partner)

    def fwd_b(g):
        return fwd(B, g, own_rows, rows(2), me + 2)

    def fwd_t(g):
        return fwd(T, g, rows(1), rows(3), me + 2)

    ahead = me + 2 < n
    behind = me >= 2
    x_in = is_odd | (me >= 2)
    x_out = is_even | (me >= 3)
    t_out = ahead & (me >= 1)
    t_in = me >= 3

    for g in range(heads):
        for c in kv_loads[g]:
            c.wait()
        @pl.when(ahead)
        def _():
            fwd_b(g).start()
        @pl.when(is_even)
        def _():
            fwd_x(g).start()

    for dist in range(1, REACH + 1):
        @pl.when(me < dist)
        def _():
            kv[:, :, (REACH - dist) * tok:(REACH - dist + 1) * tok, :] = jnp.zeros(
                (heads, 2, tok, HEAD), kv.dtype)

    window = (REACH + 1) * tok
    key_pos = (me - REACH) * tok + lax.broadcasted_iota(jnp.int32, (window, tok), 0)
    query_pos = me * tok + lax.broadcasted_iota(jnp.int32, (window, tok), 1)

    doc_load.wait()
    end = jnp.int32(0)
    crossed = jnp.zeros((window, tok), jnp.int32)
    def count(d, carry):
        end, crossed = carry
        end = end + doc_ref[d]
        return end, crossed + jnp.where((key_pos < end) & (query_pos >= end), 1, 0)
    if docs <= 8:
        for d in range(docs):
            end, crossed = count(d, (end, crossed))
    else:
        end, crossed = lax.fori_loop(0, docs, count, (end, crossed))
    allowed = (crossed == 0) & (key_pos <= query_pos) & (key_pos >= 0)
    bias[...] = jnp.where(allowed, 0.0, MASKED)

    def relay_x(g):
        @pl.when(behind)
        def _():
            fwd_b(g).wait_recv()
        @pl.when(is_odd & (me >= 3))
        def _():
            fwd_x(g).start()

    def relay_t(g):
        @pl.when(x_in)
        def _():
            fwd_x(g).wait_recv()
        @pl.when(t_out)
        def _():
            fwd_t(g).start()

    def arrive(g):
        @pl.when(t_in)
        def _():
            fwd_t(g).wait_recv()

    def bwd(kind, g, src_rows, to):
        return pltpu.make_async_remote_copy(
            src_ref=part.at[g, :, src_rows], dst_ref=back.at[kind, g],
            send_sem=bs_sem.at[kind, g], recv_sem=br_sem.at[kind, g],
            device_id={"cp": to}, device_id_type=MESH,
        )

    def bwd_x(g):
        return bwd(X, g, rows(1), partner)

    def bwd_b(g):
        return bwd(B, g, rows(2), me - 2)

    def bwd_t(g):
        return bwd(T, g, rows(3), me - 2)

    score_scale = 1.0 / math.sqrt(HEAD)
    exp_scale = score_scale * math.log2(math.e)
    nt = (((1,), (1,)), ((), ()))
    width = group * tok

    def compute(g):
        keys = kv[g, 0]
        values = kv[g, 1]
        keys_t = keys.T
        values_t = values.T
        mask = jnp.concatenate([bias[...]] * group, axis=1)
        h0 = g * group
        for h in range(h0, h0 + group):
            for c in q_loads[h]:
                c.wait()
        qs = qb[h0:h0 + group].reshape(width, HEAD)
        ds = db[h0:h0 + group].reshape(width, HEAD)
        scores = lax.dot_general(keys, qs, nt, preferred_element_type=jnp.float32) + mask
        top = jnp.max(scores, axis=0, keepdims=True)
        raw = jnp.exp2((scores - top) * exp_scale)
        probs = raw * (1.0 / jnp.sum(raw, axis=0, keepdims=True))
        low = probs.astype(jnp.bfloat16)
        att_t = jnp.dot(values_t, low, preferred_element_type=jnp.float32)
        grad_p = lax.dot_general(values, ds, nt, preferred_element_type=jnp.float32)
        delta = jnp.sum(probs * grad_p, axis=0, keepdims=True)
        grad_s = (probs * (grad_p - delta)).astype(jnp.bfloat16)
        grad_v = jnp.dot(low, ds, preferred_element_type=jnp.float32)
        grad_k = jnp.dot(grad_s, qs, preferred_element_type=jnp.float32)
        gq_t = jnp.dot(keys_t, grad_s, preferred_element_type=jnp.float32) * score_scale
        for j in range(group):
            h = h0 + j
            o_ref[:, cols(h)] = att_t[:, j * tok:(j + 1) * tok].T.astype(o_ref.dtype)
            gq_ref[:, cols(h)] = gq_t[:, j * tok:(j + 1) * tok].T.astype(gq_ref.dtype)
        for t, grad in enumerate((grad_k * score_scale, grad_v)):
            part[g, t] = grad[:REACH * tok].astype(part.dtype)
            mid[g, t] = grad[tok:REACH * tok]
            own[g, t] = grad[REACH * tok:]

    def back_t(g):
        @pl.when(t_in)
        def _():
            bwd_t(g).start()
        @pl.when(is_even & behind)
        def _():
            bwd_b(g).start()

    def back_x(g):
        @pl.when(t_out)
        def _():
            bwd_t(g).wait_recv()
            part[g, :, 2 * tok:] = (
                mid[g, :, tok:] + back[T, g].astype(jnp.float32)).astype(part.dtype)
        @pl.when(x_in)
        def _():
            bwd_x(g).start()

    def back_b(g):
        @pl.when(is_odd & (me >= 3))
        def _():
            bwd_x(g).wait_recv()
            part[g, :, tok:2 * tok] = (
                mid[g, :, :tok] + back[X, g].astype(jnp.float32)).astype(part.dtype)
            bwd_b(g).start()

    def finish(g):
        @pl.when(is_even)
        def _():
            bwd_x(g).wait_recv()
            own[g] = own[g] + back[X, g].astype(jnp.float32)
        @pl.when(ahead)
        def _():
            bwd_b(g).wait_recv()
            own[g] = own[g] + back[B, g].astype(jnp.float32)
        gk_ref[:, cols(g)] = own[g, 0].astype(gk_ref.dtype)
        gv_ref[:, cols(g)] = own[g, 1].astype(gv_ref.dtype)

    relay_x(0)
    if heads > 1:
        relay_x(1)
    relay_t(0)
    for g in range(heads + REACH):
        if g < heads:
            if g + 2 < heads:
                relay_x(g + 2)
            if g + 1 < heads:
                relay_t(g + 1)
            arrive(g)
            compute(g)
            back_t(g)
        for lag, stage in enumerate((back_x, back_b, finish)):
            if 0 <= g - 1 - lag < heads:
                stage(g - 1 - lag)

    for g in range(heads):
        for cond, copies in (
            (ahead, (fwd_b,)), (x_out, (fwd_x,)), (t_out, (fwd_t,)),
            (behind, (bwd_b,)), (x_in, (bwd_x,)), (t_in, (bwd_t,)),
        ):
            @pl.when(cond)
            def _():
                for f in copies:
                    f(g).wait_send()


def put_out(*refs):
    sems = refs[-1]
    copies = [
        pltpu.make_async_copy(refs[t], refs[4 + t], sems.at[t]) for t in range(4)
    ]
    for c in copies:
        c.start()
    for c in copies:
        c.wait()


def shards(doc_lengths, queries, key_states, value_head_states, out_grad):
    tok = queries.shape[0]
    heads = key_states.shape[1] // HEAD
    q_heads = queries.shape[1] // HEAD
    n = lax.axis_size("cp")
    window = (REACH + 1) * tok
    bf16, f32 = jnp.bfloat16, jnp.float32
    hbm_spec = pl.BlockSpec(memory_space=pltpu.HBM)
    any_spec = pl.BlockSpec(memory_space=pl.ANY)
    dma = pltpu.SemaphoreType.DMA
    args = [
        pltpu.with_memory_space_constraint(x, pltpu.HBM)
        for x in (doc_lengths, queries, key_states, value_head_states, out_grad)
    ]
    outs = pl.pallas_call(
        functools.partial(kernel, n, doc_lengths.shape[0]),
        out_shape=[
            jax.ShapeDtypeStruct(queries.shape, bf16),
            jax.ShapeDtypeStruct(queries.shape, bf16),
            jax.ShapeDtypeStruct(key_states.shape, bf16),
            jax.ShapeDtypeStruct(key_states.shape, bf16),
        ],
        in_specs=[hbm_spec] * 5,
        out_specs=[pl.BlockSpec(memory_space=pltpu.VMEM)] * 4,
        scratch_shapes=[
            pltpu.VMEM((heads, 2, window, HEAD), bf16),
            pltpu.VMEM((q_heads, tok, HEAD), bf16),
            pltpu.VMEM((q_heads, tok, HEAD), bf16),
            pltpu.VMEM((heads, 2, tok, HEAD), f32),
            pltpu.VMEM((heads, 2, 2 * tok, HEAD), f32),
            pltpu.VMEM((heads, 2, REACH * tok, HEAD), bf16),
            pltpu.VMEM((3, heads, 2, tok, HEAD), bf16),
            pltpu.VMEM((window, tok), f32),
            pltpu.SMEM(doc_lengths.shape, jnp.int32),
            dma(()),
            dma((heads, 2)),
            dma((2, q_heads)),
            dma((3, heads)),
            dma((3, heads)),
            dma((3, heads)),
            dma((3, heads)),
        ],
        compiler_params=pltpu.CompilerParams(
            collective_id=0, has_side_effects=True, vmem_limit_bytes=24 * 2**20),
        name="attend",
    )(*args)
    return tuple(pl.pallas_call(
        put_out,
        out_shape=[jax.ShapeDtypeStruct(x.shape, x.dtype) for x in outs],
        in_specs=[any_spec] * 4,
        out_specs=[hbm_spec] * 4,
        scratch_shapes=[dma((4,))],
        compiler_params=pltpu.CompilerParams(vmem_limit_bytes=2**20),
        name="put_out",
    )(*outs))


def solution(mesh):
    wide = P(("group", "cp"), "hd")
    return jax.shard_map(
        shards,
        mesh=mesh,
        in_specs=(P("group"), wide, wide, wide, wide),
        out_specs=(wide, wide, wide, wide),
        check_vma=False,
    )
```

```python
import functools
import math

import jax
import jax.numpy as jnp
from jax import lax
from jax.experimental import pallas as pl
from jax.experimental.pallas import tpu as pltpu
from jax.sharding import PartitionSpec as P

HEAD = 128
REACH = 3
MASKED = -1e30
MESH = pl.DeviceIdType.MESH
X, B, T, F = range(4)


def kernel(
    n, docs, doc_hbm, q_hbm, k_hbm, v_hbm, do_hbm, o_ref, gq_ref, gk_ref, gv_ref,
    kv, qd, own, mid, part, back, bias, doc_ref,
    doc_sem, kv_sem, q_sem, fs_sem, fr_sem, bs_sem, br_sem,
):
    tok = q_hbm.shape[0]
    heads = k_hbm.shape[1] // HEAD
    group = q_hbm.shape[1] // k_hbm.shape[1]
    me = lax.axis_index("cp")
    odd = lax.rem(me, 2)
    is_odd = odd == 1
    is_even = odd == 0
    partner = me + 1 - 2 * odd
    own_rows = pl.ds(REACH * tok, tok)

    def rows(dist):
        return pl.ds((REACH - dist) * tok, tok)

    def cols(h):
        return pl.ds(h * HEAD, HEAD)

    doc_load = pltpu.make_async_copy(doc_hbm, doc_ref, doc_sem)
    doc_load.start()
    kv_loads = []
    for g in range(heads):
        kv_loads.append([
            pltpu.make_async_copy(src.at[:, cols(g)], kv.at[g, t, own_rows], kv_sem.at[g, t])
            for t, src in enumerate((k_hbm, v_hbm))
        ])
        for c in kv_loads[g]:
            c.start()
    for h in range(heads * group):
        for t, src in enumerate((q_hbm, do_hbm)):
            pltpu.make_async_copy(
                src.at[:, cols(h)], qd.at[t, h], q_sem.at[h // group]).start()

    barrier = pltpu.get_barrier_semaphore()
    across = me - 1 + 2 * odd
    for to, cond in (
        (me - 2, me >= 2), (me + 2, me + 2 < n), (partner, me >= 0),
        (across, (across >= 1) & (across < n)),
    ):
        @pl.when(cond)
        def _():
            pl.semaphore_signal(barrier, inc=1, device_id={"cp": to}, device_id_type=MESH)
    pl.semaphore_wait(
        barrier,
        1 + jnp.minimum(me // 2, 1) + jnp.minimum((n - 1 - me) // 2, 1)
        + jnp.where((across >= 1) & (across < n), 1, 0))


    def fwd(kind, g, t, src_rows, dst_rows, to):
        return pltpu.make_async_remote_copy(
            src_ref=kv.at[g, t, src_rows], dst_ref=kv.at[g, t, dst_rows],
            send_sem=fs_sem.at[kind], recv_sem=fr_sem.at[kind, g, t],
            device_id={"cp": to}, device_id_type=MESH,
        )

    def drain(sem, block):
        pltpu.make_async_remote_copy(
            src_ref=block, dst_ref=block, send_sem=sem, recv_sem=fr_sem.at[X, 0, 0],
            device_id={"cp": partner}, device_id_type=MESH,
        ).wait_send()

    def fwd_x(g, t):
        return fwd(X, g, t, pl.ds((REACH - 2 * odd) * tok, tok), rows(1), partner)

    def fwd_b(g, t):
        return fwd(B, g, t, own_rows, rows(2), me + 2)

    def fwd_t(g, t):
        return fwd(T, g, t, rows(1), rows(3), me + 2)

    ahead = me + 2 < n
    behind = me >= 2
    x_in = is_odd | (me >= 2)
    x_out = is_even | (me >= 3)
    t_out = ahead & (me >= 1)
    t_in = me >= 3
    parts = [(g, t) for g in range(heads) for t in range(2)]

    last = heads - 1
    for g, t in parts:
        kv_loads[g][t].wait()
        @pl.when(ahead)
        def _():
            fwd_b(g, t).start()
        @pl.when(is_even)
        def _():
            fwd_x(g, t).start()

    for dist in range(1, REACH + 1):
        @pl.when(me < dist)
        def _():
            kv[:, :, (REACH - dist) * tok:(REACH - dist + 1) * tok, :] = jnp.zeros(
                (heads, 2, tok, HEAD), kv.dtype)

    window = (REACH + 1) * tok
    key_pos = (me - REACH) * tok + lax.broadcasted_iota(jnp.int32, (window, tok), 0)
    query_pos = me * tok + lax.broadcasted_iota(jnp.int32, (window, tok), 1)

    doc_load.wait()
    end = jnp.int32(0)
    crossed = jnp.zeros((window, tok), jnp.int32)
    def count(d, carry):
        end, crossed = carry
        end = end + doc_ref[d]
        return end, crossed + jnp.where((key_pos < end) & (query_pos >= end), 1, 0)
    if docs <= 8:
        for d in range(docs):
            end, crossed = count(d, (end, crossed))
    else:
        end, crossed = lax.fori_loop(0, docs, count, (end, crossed))
    allowed = (crossed == 0) & (key_pos <= query_pos) & (key_pos >= 0)
    bias[...] = jnp.where(allowed, 0.0, MASKED)

    def relay_x(g, t):
        @pl.when(behind)
        def _():
            fwd_b(g, t).wait_recv()
        @pl.when(is_odd & (me >= 3))
        def _():
            fwd_x(g, t).start()

    def x_arrive(g, t):
        @pl.when(is_odd)
        def _():
            fwd_x(g, t).wait_recv()
        @pl.when(is_odd & ahead)
        def _():
            fwd_t(g, t).start()

    def relay_t(g, t):
        @pl.when(is_even & behind)
        def _():
            fwd_x(g, t).wait_recv()
        @pl.when(is_even & t_out)
        def _():
            fwd_t(g, t).start()

    def arrive(g):
        @pl.when(t_in)
        def _():
            for t in range(2):
                fwd_t(g, t).wait_recv()

    def bwd(kind, g, t, src_rows, to):
        return pltpu.make_async_remote_copy(
            src_ref=part.at[g, t, src_rows], dst_ref=back.at[kind, g, t],
            send_sem=bs_sem.at[min(kind, T)], recv_sem=br_sem.at[kind, g, t],
            device_id={"cp": to}, device_id_type=MESH,
        )

    def bwd_x(g, t):
        return bwd(X, g, t, rows(1), partner)

    def bwd_b(g, t):
        return bwd(B, g, t, rows(2), me - 2)

    def bwd_t(g, t):
        return bwd(T, g, t, rows(3), me - 2)

    def bwd_f(g, t):
        return bwd(F, g, t, rows(3), me - 1)

    score_scale = 1.0 / math.sqrt(HEAD)
    exp_scale = score_scale * math.log2(math.e)
    nt = (((1,), (1,)), ((), ()))
    width = group * tok

    def compute(g):
        keys = kv[g, 0]
        values = kv[g, 1]
        keys_t = keys.T
        values_t = values.T
        mask = jnp.concatenate([bias[...]] * group, axis=1)
        h0 = g * group
        loaded = qd.at[:, h0:h0 + group]
        pltpu.make_async_copy(loaded, loaded, q_sem.at[g]).wait()
        qs = qd[0, h0:h0 + group].reshape(width, HEAD)
        ds = qd[1, h0:h0 + group].reshape(width, HEAD)
        scores = lax.dot_general(keys, qs, nt, preferred_element_type=jnp.float32) + mask
        top = jnp.max(scores, axis=0, keepdims=True)
        raw = jnp.exp2((scores - top) * exp_scale)
        probs = raw * (1.0 / jnp.sum(raw, axis=0, keepdims=True))
        low = probs.astype(jnp.bfloat16)
        att_t = jnp.dot(values_t, low, preferred_element_type=jnp.float32)
        grad_p = lax.dot_general(values, ds, nt, preferred_element_type=jnp.float32)
        delta = jnp.sum(probs * grad_p, axis=0, keepdims=True)
        grad_s = (probs * (grad_p - delta)).astype(jnp.bfloat16)
        grad_v = jnp.dot(low, ds, preferred_element_type=jnp.float32)
        grad_k = jnp.dot(grad_s, qs, preferred_element_type=jnp.float32)
        gq_t = jnp.dot(keys_t, grad_s, preferred_element_type=jnp.float32) * score_scale
        for j in range(group):
            h = h0 + j
            o_ref[:, cols(h)] = att_t[:, j * tok:(j + 1) * tok].T.astype(o_ref.dtype)
            gq_ref[:, cols(h)] = gq_t[:, j * tok:(j + 1) * tok].T.astype(gq_ref.dtype)
        for t, grad in enumerate((grad_k * score_scale, grad_v)):
            part[g, t] = grad[:REACH * tok].astype(part.dtype)
            mid[g, t] = grad[tok:REACH * tok]
            own[g, t] = grad[REACH * tok:]

    def back_start(g):
        @pl.when(t_in & is_odd)
        def _():
            for t in range(2):
                bwd_t(g, t).start()
        @pl.when(t_in & is_even)
        def _():
            for t in range(2):
                bwd_f(g, t).start()
        @pl.when(is_even & behind)
        def _():
            for t in range(2):
                bwd_x(g, t).start()
            for t in range(2):
                bwd_b(g, t).start()

    def back_x(g, t):
        @pl.when(is_odd & ahead)
        def _():
            bwd_t(g, t).wait_recv()
            part[g, t, 2 * tok:] = (
                mid[g, t, tok:] + back[T, g, t].astype(jnp.float32)).astype(part.dtype)
        @pl.when(is_odd)
        def _():
            bwd_x(g, t).start()

    def back_b(g, t):
        passes = is_odd & (me >= 3)
        @pl.when(passes)
        def _():
            bwd_x(g, t).wait_recv()
            mid[g, t, :tok] = mid[g, t, :tok] + back[X, g, t].astype(jnp.float32)
        far_in(g, t)
        @pl.when(passes)
        def _():
            part[g, t, tok:2 * tok] = mid[g, t, :tok].astype(part.dtype)
            bwd_b(g, t).start()

    def far_in(g, t):
        @pl.when(is_odd & (me >= 3) & (me + 1 < n))
        def _():
            bwd_f(g, t).wait_recv()
            mid[g, t, :tok] = mid[g, t, :tok] + back[F, g, t].astype(jnp.float32)

    def finish(g, t):
        @pl.when(is_even)
        def _():
            bwd_x(g, t).wait_recv()
            own[g, t] = own[g, t] + back[X, g, t].astype(jnp.float32)
        @pl.when(ahead)
        def _():
            bwd_b(g, t).wait_recv()
            own[g, t] = own[g, t] + back[B, g, t].astype(jnp.float32)
        out = gv_ref if t else gk_ref
        out[:, cols(g)] = own[g, t].astype(out.dtype)

    for g, t in parts:
        relay_x(g, t)
        x_arrive(g, t)
    for g, t in parts[:-2]:
        relay_t(g, t)
    for g in range(heads):
        arrive(g)
        compute(g)
        back_start(g)
        if g == 0:
            for t in range(2):
                relay_t(last, t)
    lag = 2
    for g in range(heads + lag):
        for t in range(2):
            if g < heads:
                back_x(g, t)
            if g >= lag:
                back_b(g - lag, t)
    for g, t in parts:
        finish(g, t)

    for cond, sem, block in (
        (ahead, fs_sem.at[B], kv.at[:, :, own_rows]),
        (x_out, fs_sem.at[X], kv.at[:, :, own_rows]),
        (t_out, fs_sem.at[T], kv.at[:, :, own_rows]),
        (behind, bs_sem.at[B], kv.at[:, :, own_rows]),
        (x_in, bs_sem.at[X], kv.at[:, :, own_rows]),
        (t_in, bs_sem.at[T], kv.at[:, :, own_rows]),
    ):
        @pl.when(cond)
        def _():
            drain(sem, block)


def put_out(*refs):
    sems = refs[-1]
    copies = [
        pltpu.make_async_copy(refs[t], refs[4 + t], sems.at[t]) for t in range(4)
    ]
    for c in copies:
        c.start()
    for c in copies:
        c.wait()


def shards(doc_lengths, queries, key_states, value_head_states, out_grad):
    tok = queries.shape[0]
    heads = key_states.shape[1] // HEAD
    q_heads = queries.shape[1] // HEAD
    n = lax.axis_size("cp")
    window = (REACH + 1) * tok
    bf16, f32 = jnp.bfloat16, jnp.float32
    hbm_spec = pl.BlockSpec(memory_space=pltpu.HBM)
    any_spec = pl.BlockSpec(memory_space=pl.ANY)
    dma = pltpu.SemaphoreType.DMA
    args = [
        pltpu.with_memory_space_constraint(x, pltpu.HBM)
        for x in (doc_lengths, queries, key_states, value_head_states, out_grad)
    ]
    outs = pl.pallas_call(
        functools.partial(kernel, n, doc_lengths.shape[0]),
        out_shape=[
            jax.ShapeDtypeStruct(queries.shape, bf16),
            jax.ShapeDtypeStruct(queries.shape, bf16),
            jax.ShapeDtypeStruct(key_states.shape, bf16),
            jax.ShapeDtypeStruct(key_states.shape, bf16),
        ],
        in_specs=[hbm_spec] * 5,
        out_specs=[pl.BlockSpec(memory_space=pltpu.VMEM)] * 4,
        scratch_shapes=[
            pltpu.VMEM((heads, 2, window, HEAD), bf16),
            pltpu.VMEM((2, q_heads, tok, HEAD), bf16),
            pltpu.VMEM((heads, 2, tok, HEAD), f32),
            pltpu.VMEM((heads, 2, 2 * tok, HEAD), f32),
            pltpu.VMEM((heads, 2, REACH * tok, HEAD), bf16),
            pltpu.VMEM((4, heads, 2, tok, HEAD), bf16),
            pltpu.VMEM((window, tok), f32),
            pltpu.SMEM(doc_lengths.shape, jnp.int32),
            dma(()),
            dma((heads, 2)),
            dma((heads,)),
            dma((3,)),
            dma((3, heads, 2)),
            dma((3,)),
            dma((4, heads, 2)),
        ],
        compiler_params=pltpu.CompilerParams(
            collective_id=0, has_side_effects=True, vmem_limit_bytes=24 * 2**20),
        name="attend",
    )(*args)
    return tuple(pl.pallas_call(
        put_out,
        out_shape=[jax.ShapeDtypeStruct(x.shape, x.dtype) for x in outs],
        in_specs=[any_spec] * 4,
        out_specs=[hbm_spec] * 4,
        scratch_shapes=[dma((4,))],
        compiler_params=pltpu.CompilerParams(vmem_limit_bytes=2**20),
        name="put_out",
    )(*outs))


def solution(mesh):
    wide = P(("group", "cp"), "hd")
    return jax.shard_map(
        shards,
        mesh=mesh,
        in_specs=(P("group"), wide, wide, wide, wide),
        out_specs=(wide, wide, wide, wide),
        check_vma=False,
    )
```

```python
import functools
import math

import jax
import jax.numpy as jnp
from jax import lax
from jax.experimental import pallas as pl
from jax.experimental.pallas import tpu as pltpu
from jax.sharding import PartitionSpec as P

HEAD = 128
REACH = 3
MASKED = -1e30
MESH = pl.DeviceIdType.MESH
X, B, T, F = range(4)


def kernel(
    n, docs, doc_hbm, q_hbm, k_hbm, v_hbm, do_hbm, o_ref, gq_ref, gk_ref, gv_ref,
    kv, qd, own, mid, part, back, low_ref, grad_ref, bias, doc_ref,
    doc_sem, kv_sem, q_sem, fs_sem, fr_sem, bs_sem, br_sem,
):
    tok = q_hbm.shape[0]
    heads = k_hbm.shape[1] // HEAD
    group = q_hbm.shape[1] // k_hbm.shape[1]
    me = lax.axis_index("cp")
    odd = lax.rem(me, 2)
    is_odd = odd == 1
    is_even = odd == 0
    partner = me + 1 - 2 * odd
    short = lax.axis_index("hd") == 0
    slow = is_odd | jnp.logical_not(short)
    own_rows = pl.ds(REACH * tok, tok)

    def rows(dist):
        return pl.ds((REACH - dist) * tok, tok)

    def cols(h):
        return pl.ds(h * HEAD, HEAD)

    doc_load = pltpu.make_async_copy(doc_hbm, doc_ref, doc_sem)
    doc_load.start()
    kv_loads = []
    for g in range(heads):
        kv_loads.append([
            pltpu.make_async_copy(src.at[:, cols(g)], kv.at[g, t, own_rows], kv_sem.at[g, t])
            for t, src in enumerate((k_hbm, v_hbm))
        ])
        for c in kv_loads[g]:
            c.start()
    for h in range(heads * group):
        for t, src in enumerate((q_hbm, do_hbm)):
            pltpu.make_async_copy(
                src.at[:, cols(h)], qd.at[t, h], q_sem.at[h // group]).start()

    barrier = pltpu.get_barrier_semaphore()
    across = me - 1 + 2 * odd
    for to, cond in (
        (me - 2, me >= 2), (me + 2, me + 2 < n), (partner, me >= 0),
        (across, (across >= 1) & (across < n)),
    ):
        @pl.when(cond)
        def _():
            pl.semaphore_signal(barrier, inc=1, device_id={"cp": to}, device_id_type=MESH)
    pl.semaphore_wait(
        barrier,
        1 + jnp.minimum(me // 2, 1) + jnp.minimum((n - 1 - me) // 2, 1)
        + jnp.where((across >= 1) & (across < n), 1, 0))


    def fwd(kind, g, t, src_rows, dst_rows, to):
        return pltpu.make_async_remote_copy(
            src_ref=kv.at[g, t, src_rows], dst_ref=kv.at[g, t, dst_rows],
            send_sem=fs_sem.at[kind], recv_sem=fr_sem.at[kind, g, t],
            device_id={"cp": to}, device_id_type=MESH,
        )

    def drain(sem, block):
        pltpu.make_async_remote_copy(
            src_ref=block, dst_ref=block, send_sem=sem, recv_sem=fr_sem.at[X, 0, 0],
            device_id={"cp": partner}, device_id_type=MESH,
        ).wait_send()

    def fwd_x(g, t):
        return fwd(X, g, t, pl.ds((REACH - 2 * odd) * tok, tok), rows(1), partner)

    def fwd_b(g, t):
        return fwd(B, g, t, own_rows, rows(2), me + 2)

    def fwd_t(g, t):
        return fwd(T, g, t, rows(1), rows(3), me + 2)

    ahead = me + 2 < n
    behind = me >= 2
    x_in = is_odd | (me >= 2)
    x_out = is_even | (me >= 3)
    t_out = ahead & (me >= 1)
    t_in = me >= 3
    parts = [(g, t) for g in range(heads) for t in range(2)]

    last = heads - 1
    early = 4

    def send_own(cond, g, t):
        @pl.when(cond & ahead)
        def _():
            fwd_b(g, t).start()
        @pl.when(cond & is_even)
        def _():
            fwd_x(g, t).start()

    for i, (g, t) in enumerate(parts):
        kv_loads[g][t].wait()
        send_own(short if i >= early else me >= 0, g, t)

    for dist in range(1, REACH + 1):
        @pl.when(me < dist)
        def _():
            kv[:, :, (REACH - dist) * tok:(REACH - dist + 1) * tok, :] = jnp.zeros(
                (heads, 2, tok, HEAD), kv.dtype)

    window = (REACH + 1) * tok
    key_pos = (me - REACH) * tok + lax.broadcasted_iota(jnp.int32, (window, tok), 0)
    query_pos = me * tok + lax.broadcasted_iota(jnp.int32, (window, tok), 1)

    doc_load.wait()
    end = jnp.int32(0)
    crossed = jnp.zeros((window, tok), jnp.int32)
    def count(d, carry):
        end, crossed = carry
        end = end + doc_ref[d]
        return end, crossed + jnp.where((key_pos < end) & (query_pos >= end), 1, 0)
    if docs <= 8:
        for d in range(docs):
            end, crossed = count(d, (end, crossed))
    else:
        end, crossed = lax.fori_loop(0, docs, count, (end, crossed))
    allowed = (crossed == 0) & (key_pos <= query_pos) & (key_pos >= 0)
    bias[...] = jnp.where(allowed, 0.0, MASKED)

    def relay_x(g, t):
        @pl.when(behind)
        def _():
            fwd_b(g, t).wait_recv()
        @pl.when(is_odd & (me >= 3))
        def _():
            fwd_x(g, t).start()

    def x_arrive(g, t):
        @pl.when(is_odd)
        def _():
            fwd_x(g, t).wait_recv()
        @pl.when(is_odd & ahead)
        def _():
            fwd_t(g, t).start()

    def relay_t(g, t, now):
        @pl.when(now & is_even & behind)
        def _():
            fwd_x(g, t).wait_recv()
        @pl.when(now & is_even & t_out)
        def _():
            fwd_t(g, t).start()

    def arrive(g):
        @pl.when(t_in)
        def _():
            for t in range(2):
                fwd_t(g, t).wait_recv()

    def bwd(kind, g, t, src_rows, to):
        return pltpu.make_async_remote_copy(
            src_ref=part.at[g, t, src_rows], dst_ref=back.at[kind, g, t],
            send_sem=bs_sem.at[min(kind, T)], recv_sem=br_sem.at[kind, g, t],
            device_id={"cp": to}, device_id_type=MESH,
        )

    def bwd_x(g, t):
        return bwd(X, g, t, rows(1), partner)

    def bwd_b(g, t):
        return bwd(B, g, t, rows(2), me - 2)

    def bwd_t(g, t):
        return bwd(T, g, t, rows(3), me - 2)

    def bwd_f(g, t):
        return bwd(F, g, t, rows(3), me - 1)

    score_scale = 1.0 / math.sqrt(HEAD)
    exp_scale = score_scale * math.log2(math.e)
    nt = (((1,), (1,)), ((), ()))
    width = group * tok

    def cotangents(t, g):
        return qd[t, g * group:(g + 1) * group].reshape(width, HEAD)

    def compute(g):
        keys = kv[g, 0]
        values = kv[g, 1]
        mask = jnp.concatenate([bias[...]] * group, axis=1)
        loaded = qd.at[:, g * group:(g + 1) * group]
        pltpu.make_async_copy(loaded, loaded, q_sem.at[g]).wait()
        qs = cotangents(0, g)
        ds = cotangents(1, g)
        scores = lax.dot_general(keys, qs, nt, preferred_element_type=jnp.float32) + mask
        top = jnp.max(scores, axis=0, keepdims=True)
        raw = jnp.exp2((scores - top) * exp_scale)
        probs = raw * (1.0 / jnp.sum(raw, axis=0, keepdims=True))
        low = probs.astype(jnp.bfloat16)
        low_ref[g] = low
        grad_p = lax.dot_general(values, ds, nt, preferred_element_type=jnp.float32)
        delta = jnp.sum(probs * grad_p, axis=0, keepdims=True)
        grad_s = (probs * (grad_p - delta)).astype(jnp.bfloat16)
        grad_ref[g] = grad_s
        grad_v = jnp.dot(low, ds, preferred_element_type=jnp.float32)
        grad_k = jnp.dot(grad_s, qs, preferred_element_type=jnp.float32)
        for t, grad in enumerate((grad_k * score_scale, grad_v)):
            part[g, t] = grad[:REACH * tok].astype(part.dtype)
            mid[g, t] = grad[tok:REACH * tok]
            own[g, t] = grad[REACH * tok:]

    def outputs(g):
        for t, weights, out, scale in ((1, low_ref, o_ref, 1.0), (0, grad_ref, gq_ref, score_scale)):
            res = jnp.dot(kv[g, t].T, weights[g], preferred_element_type=jnp.float32) * scale
            for j in range(group):
                out[:, cols(g * group + j)] = (
                    res[:, j * tok:(j + 1) * tok].T.astype(out.dtype))

    def back_start(g):
        for cond, f in (
            (t_in & slow, bwd_t), (t_in & is_even & short, bwd_f), (is_even & behind & short, bwd_x),
        ):
            @pl.when(cond)
            def _():
                for t in range(2):
                    f(g, t).start()

    def back_even(cond):
        @pl.when(is_even & behind & cond)
        def _():
            for g, t in parts:
                bwd_b(g, t).start()

    def back_x(g, t, now):
        @pl.when(now & slow & t_out)
        def _():
            bwd_t(g, t).wait_recv()
            part[g, t, 2 * tok:] = (
                mid[g, t, tok:] + back[T, g, t].astype(jnp.float32)).astype(part.dtype)
        @pl.when(now & slow & x_in)
        def _():
            bwd_x(g, t).start()

    def back_b(g, t):
        passes = is_odd & (me >= 3)
        @pl.when(passes)
        def _():
            bwd_x(g, t).wait_recv()
            mid[g, t, :tok] = mid[g, t, :tok] + back[X, g, t].astype(jnp.float32)
        far_in(g, t)
        @pl.when(passes)
        def _():
            part[g, t, tok:2 * tok] = mid[g, t, :tok].astype(part.dtype)
            bwd_b(g, t).start()

    def far_in(g, t):
        @pl.when(is_odd & (me >= 3) & (me + 1 < n) & short)
        def _():
            bwd_f(g, t).wait_recv()
            mid[g, t, :tok] = mid[g, t, :tok] + back[F, g, t].astype(jnp.float32)

    def finish(g, t):
        @pl.when(is_even)
        def _():
            bwd_x(g, t).wait_recv()
            own[g, t] = own[g, t] + back[X, g, t].astype(jnp.float32)
        @pl.when(ahead)
        def _():
            bwd_b(g, t).wait_recv()
            own[g, t] = own[g, t] + back[B, g, t].astype(jnp.float32)
        out = gv_ref if t else gk_ref
        out[:, cols(g)] = own[g, t].astype(out.dtype)

    for i, (g, t) in enumerate(parts):
        relay_x(g, t)
        if i + early < len(parts):
            send_own(jnp.logical_not(short), *parts[i + early])
        x_arrive(g, t)
    for g, t in parts[:-2]:
        relay_t(g, t, me >= 0)
    for g in range(heads):
        arrive(g)
        compute(g)
        back_start(g)
        for when, core in ((0, short), (min(1, last), jnp.logical_not(short))):
            if g == when:
                for t in range(2):
                    relay_t(last, t, core)
    back_even(short)
    ahead_of = 2 if heads > 1 else 1
    for h in range(heads):
        for t in range(2):
            back_x(h, t, me >= 0)
        if h == 0:
            for g in range(ahead_of):
                outputs(g)
            continue
        for t in range(2):
            back_b(h - 1, t)
        if h + 1 < heads:
            outputs(h + 1)
        if h + 2 == heads:
            back_even(jnp.logical_not(short))
    if heads < 2:
        back_even(jnp.logical_not(short))
    for t in range(2):
        back_b(last, t)
    for g, t in parts:
        finish(g, t)

    for cond, sem, block in (
        (ahead, fs_sem.at[B], kv.at[:, :, own_rows]),
        (x_out, fs_sem.at[X], kv.at[:, :, own_rows]),
        (t_out, fs_sem.at[T], kv.at[:, :, own_rows]),
        (behind, bs_sem.at[B], kv.at[:, :, own_rows]),
        (x_in, bs_sem.at[X], kv.at[:, :, own_rows]),
        (t_in, bs_sem.at[T], kv.at[:, :, own_rows]),
    ):
        @pl.when(cond)
        def _():
            drain(sem, block)


def put_out(*refs):
    sems = refs[-1]
    copies = [
        pltpu.make_async_copy(refs[t], refs[4 + t], sems.at[t]) for t in range(4)
    ]
    for c in copies:
        c.start()
    for c in copies:
        c.wait()


def shards(doc_lengths, queries, key_states, value_head_states, out_grad):
    tok = queries.shape[0]
    heads = key_states.shape[1] // HEAD
    q_heads = queries.shape[1] // HEAD
    n = lax.axis_size("cp")
    window = (REACH + 1) * tok
    bf16, f32 = jnp.bfloat16, jnp.float32
    hbm_spec = pl.BlockSpec(memory_space=pltpu.HBM)
    any_spec = pl.BlockSpec(memory_space=pl.ANY)
    dma = pltpu.SemaphoreType.DMA
    args = [
        pltpu.with_memory_space_constraint(x, pltpu.HBM)
        for x in (doc_lengths, queries, key_states, value_head_states, out_grad)
    ]
    outs = pl.pallas_call(
        functools.partial(kernel, n, doc_lengths.shape[0]),
        out_shape=[
            jax.ShapeDtypeStruct(queries.shape, bf16),
            jax.ShapeDtypeStruct(queries.shape, bf16),
            jax.ShapeDtypeStruct(key_states.shape, bf16),
            jax.ShapeDtypeStruct(key_states.shape, bf16),
        ],
        in_specs=[hbm_spec] * 5,
        out_specs=[pl.BlockSpec(memory_space=pltpu.VMEM)] * 4,
        scratch_shapes=[
            pltpu.VMEM((heads, 2, window, HEAD), bf16),
            pltpu.VMEM((2, q_heads, tok, HEAD), bf16),
            pltpu.VMEM((heads, 2, tok, HEAD), f32),
            pltpu.VMEM((heads, 2, 2 * tok, HEAD), f32),
            pltpu.VMEM((heads, 2, REACH * tok, HEAD), bf16),
            pltpu.VMEM((4, heads, 2, tok, HEAD), bf16),
            pltpu.VMEM((heads, window, q_heads // heads * tok), bf16),
            pltpu.VMEM((heads, window, q_heads // heads * tok), bf16),
            pltpu.VMEM((window, tok), f32),
            pltpu.SMEM(doc_lengths.shape, jnp.int32),
            dma(()),
            dma((heads, 2)),
            dma((heads,)),
            dma((3,)),
            dma((3, heads, 2)),
            dma((3,)),
            dma((4, heads, 2)),
        ],
        compiler_params=pltpu.CompilerParams(
            collective_id=0, has_side_effects=True, vmem_limit_bytes=24 * 2**20),
        name="attend",
    )(*args)
    return tuple(pl.pallas_call(
        put_out,
        out_shape=[jax.ShapeDtypeStruct(x.shape, x.dtype) for x in outs],
        in_specs=[any_spec] * 4,
        out_specs=[hbm_spec] * 4,
        scratch_shapes=[dma((4,))],
        compiler_params=pltpu.CompilerParams(vmem_limit_bytes=2**20),
        name="put_out",
    )(*outs))


def solution(mesh):
    wide = P(("group", "cp"), "hd")
    return jax.shard_map(
        shards,
        mesh=mesh,
        in_specs=(P("group"), wide, wide, wide, wide),
        out_specs=(wide, wide, wide, wide),
        check_vma=False,
    )
```

```python
import functools
import math

import jax
import jax.numpy as jnp
from jax import lax
from jax.experimental import pallas as pl
from jax.experimental.pallas import tpu as pltpu
from jax.sharding import PartitionSpec as P

HEAD = 128
REACH = 3
MASKED = -1e30
MESH = pl.DeviceIdType.MESH
X, B, T = range(3)


def kernel(
    n, docs, doc_hbm, q_hbm, k_hbm, v_hbm, do_hbm, o_ref, gq_ref, gk_ref, gv_ref,
    kv, qd, own, mid, part, back, low_ref, grad_ref, bias, doc_ref,
    doc_sem, kv_sem, q_sem, fs_sem, fr_sem, bs_sem, br_sem,
):
    tok = q_hbm.shape[0]
    heads = k_hbm.shape[1] // HEAD
    group = q_hbm.shape[1] // k_hbm.shape[1]
    me = lax.axis_index("cp")
    odd = lax.rem(me, 2)
    is_odd = odd == 1
    is_even = odd == 0
    partner = me + 1 - 2 * odd
    short = lax.axis_index("hd") == 0
    own_rows = pl.ds(REACH * tok, tok)

    def rows(dist):
        return pl.ds((REACH - dist) * tok, tok)

    def cols(h):
        return pl.ds(h * HEAD, HEAD)

    doc_load = pltpu.make_async_copy(doc_hbm, doc_ref, doc_sem)
    doc_load.start()
    kv_loads = []
    for g in range(heads):
        kv_loads.append([
            pltpu.make_async_copy(src.at[:, cols(g)], kv.at[g, t, own_rows], kv_sem.at[g, t])
            for t, src in enumerate((k_hbm, v_hbm))
        ])
        for c in kv_loads[g]:
            c.start()
    for h in range(heads * group):
        for t, src in enumerate((q_hbm, do_hbm)):
            pltpu.make_async_copy(
                src.at[:, cols(h)], qd.at[t, h], q_sem.at[h // group]).start()

    barrier = pltpu.get_barrier_semaphore()
    for to, cond in ((me - 2, me >= 2), (me + 2, me + 2 < n), (partner, me >= 0)):
        @pl.when(cond)
        def _():
            pl.semaphore_signal(barrier, inc=1, device_id={"cp": to}, device_id_type=MESH)
    pl.semaphore_wait(
        barrier,
        1 + jnp.minimum(me // 2, 1) + jnp.minimum((n - 1 - me) // 2, 1))


    def fwd(kind, g, t, src_rows, dst_rows, to):
        return pltpu.make_async_remote_copy(
            src_ref=kv.at[g, t, src_rows], dst_ref=kv.at[g, t, dst_rows],
            send_sem=fs_sem.at[kind], recv_sem=fr_sem.at[kind, g, t],
            device_id={"cp": to}, device_id_type=MESH,
        )

    def drain(sem, block):
        pltpu.make_async_remote_copy(
            src_ref=block, dst_ref=block, send_sem=sem, recv_sem=fr_sem.at[X, 0, 0],
            device_id={"cp": partner}, device_id_type=MESH,
        ).wait_send()

    def fwd_x(g, t):
        return fwd(X, g, t, pl.ds((REACH - 2 * odd) * tok, tok), rows(1), partner)

    def fwd_b(g, t):
        return fwd(B, g, t, own_rows, rows(2), me + 2)

    def fwd_t(g, t):
        return fwd(T, g, t, rows(1), rows(3), me + 2)

    ahead = me + 2 < n
    behind = me >= 2
    x_in = is_odd | (me >= 2)
    x_out = is_even | (me >= 3)
    t_out = ahead & (me >= 1)
    t_in = me >= 3
    parts = [(g, t) for g in range(heads) for t in range(2)]
    turned = [(g, 1 - t) for g, t in parts]

    last = heads - 1
    early = 4

    def send_own(cond, g, t):
        @pl.when(cond & ahead)
        def _():
            fwd_b(g, t).start()
        @pl.when(cond & is_even)
        def _():
            fwd_x(g, t).start()

    for i, (g, t) in enumerate(parts):
        kv_loads[g][t].wait()
        send_own(short if i >= early else me >= 0, g, t)

    for dist in range(1, REACH + 1):
        @pl.when(me < dist)
        def _():
            kv[:, :, (REACH - dist) * tok:(REACH - dist + 1) * tok, :] = jnp.zeros(
                (heads, 2, tok, HEAD), kv.dtype)

    window = (REACH + 1) * tok
    key_pos = (me - REACH) * tok + lax.broadcasted_iota(jnp.int32, (window, tok), 0)
    query_pos = me * tok + lax.broadcasted_iota(jnp.int32, (window, tok), 1)

    doc_load.wait()
    end = jnp.int32(0)
    crossed = jnp.zeros((window, tok), jnp.int32)
    def count(d, carry):
        end, crossed = carry
        end = end + doc_ref[d]
        return end, crossed + jnp.where((key_pos < end) & (query_pos >= end), 1, 0)
    if docs <= 8:
        for d in range(docs):
            end, crossed = count(d, (end, crossed))
    else:
        end, crossed = lax.fori_loop(0, docs, count, (end, crossed))
    allowed = (crossed == 0) & (key_pos <= query_pos) & (key_pos >= 0)
    bias[...] = jnp.where(allowed, 0.0, MASKED)

    def relay_x(g, t):
        @pl.when(behind)
        def _():
            fwd_b(g, t).wait_recv()
        @pl.when(is_odd & (me >= 3))
        def _():
            fwd_x(g, t).start()

    def x_arrive(g, t):
        @pl.when(is_odd)
        def _():
            fwd_x(g, t).wait_recv()
        @pl.when(is_odd & ahead)
        def _():
            fwd_t(g, t).start()

    def relay_t(g, t, now):
        @pl.when(now & is_even & behind)
        def _():
            fwd_x(g, t).wait_recv()
        @pl.when(now & is_even & t_out)
        def _():
            fwd_t(g, t).start()

    def arrive(g):
        @pl.when(t_in)
        def _():
            for t in range(2):
                fwd_t(g, t).wait_recv()

    def bwd(kind, g, t, src_rows, to):
        return pltpu.make_async_remote_copy(
            src_ref=part.at[g, t, src_rows], dst_ref=back.at[kind, g, t],
            send_sem=bs_sem.at[kind], recv_sem=br_sem.at[kind, g, t],
            device_id={"cp": to}, device_id_type=MESH,
        )

    def bwd_x(g, t):
        return bwd(X, g, t, rows(1), partner)

    def bwd_b(g, t):
        return bwd(B, g, t, rows(2), me - 2)

    def bwd_t(g, t):
        return bwd(T, g, t, rows(3), me - 2)

    score_scale = 1.0 / math.sqrt(HEAD)
    exp_scale = score_scale * math.log2(math.e)
    nt = (((1,), (1,)), ((), ()))
    width = group * tok

    def cotangents(t, g):
        return qd[t, g * group:(g + 1) * group].reshape(width, HEAD)

    def compute(g):
        keys = kv[g, 0]
        values = kv[g, 1]
        mask = jnp.concatenate([bias[...]] * group, axis=1)
        loaded = qd.at[:, g * group:(g + 1) * group]
        pltpu.make_async_copy(loaded, loaded, q_sem.at[g]).wait()
        qs = cotangents(0, g)
        ds = cotangents(1, g)
        scores = lax.dot_general(keys, qs, nt, preferred_element_type=jnp.float32) + mask
        top = jnp.max(scores, axis=0, keepdims=True)
        raw = jnp.exp2((scores - top) * exp_scale)
        probs = raw * (1.0 / jnp.sum(raw, axis=0, keepdims=True))
        low = probs.astype(jnp.bfloat16)
        low_ref[g] = low
        keep(g, 1, jnp.dot(low, ds, preferred_element_type=jnp.float32))
        back_start(g, 1)
        grad_p = lax.dot_general(values, ds, nt, preferred_element_type=jnp.float32)
        delta = jnp.sum(probs * grad_p, axis=0, keepdims=True)
        grad_s = (probs * (grad_p - delta)).astype(jnp.bfloat16)
        grad_ref[g] = grad_s
        keep(g, 0, jnp.dot(grad_s, qs, preferred_element_type=jnp.float32) * score_scale)
        back_start(g, 0)

    def keep(g, t, grad):
        part[g, t] = grad[:REACH * tok].astype(part.dtype)
        mid[g, t] = grad[tok:REACH * tok]
        own[g, t] = grad[REACH * tok:]

    def outputs(g):
        for t, weights, out, scale in ((1, low_ref, o_ref, 1.0), (0, grad_ref, gq_ref, score_scale)):
            res = jnp.dot(kv[g, t].T, weights[g], preferred_element_type=jnp.float32) * scale
            for j in range(group):
                out[:, cols(g * group + j)] = (
                    res[:, j * tok:(j + 1) * tok].T.astype(out.dtype))

    def back_start(g, t):
        @pl.when(t_in)
        def _():
            bwd_t(g, t).start()

    def back_even(cond):
        @pl.when(is_even & behind & cond)
        def _():
            for g, t in turned:
                bwd_b(g, t).start()

    def back_x(g, t):
        @pl.when(t_out)
        def _():
            bwd_t(g, t).wait_recv()
            part[g, t, 2 * tok:] = (
                mid[g, t, tok:] + back[T, g, t].astype(jnp.float32)).astype(part.dtype)
        @pl.when(x_in)
        def _():
            bwd_x(g, t).start()

    def back_b(g, t):
        @pl.when(is_odd & (me >= 3))
        def _():
            bwd_x(g, t).wait_recv()
            part[g, t, tok:2 * tok] = (
                mid[g, t, :tok] + back[X, g, t].astype(jnp.float32)).astype(part.dtype)
            bwd_b(g, t).start()

    def finish(g, t):
        @pl.when(is_even)
        def _():
            bwd_x(g, t).wait_recv()
            own[g, t] = own[g, t] + back[X, g, t].astype(jnp.float32)
        @pl.when(ahead)
        def _():
            bwd_b(g, t).wait_recv()
            own[g, t] = own[g, t] + back[B, g, t].astype(jnp.float32)
        out = gv_ref if t else gk_ref
        out[:, cols(g)] = own[g, t].astype(out.dtype)

    for i, (g, t) in enumerate(parts):
        relay_x(g, t)
        if i + early < len(parts):
            send_own(jnp.logical_not(short), *parts[i + early])
        x_arrive(g, t)
    for g, t in parts[:-2]:
        relay_t(g, t, me >= 0)
    for g in range(heads):
        arrive(g)
        compute(g)
        for when, core in ((0, short), (min(1, last), jnp.logical_not(short))):
            if g == when:
                for t in range(2):
                    relay_t(last, t, core)
    back_even(short)
    for h in range(heads):
        for t in (1, 0):
            back_x(h, t)
        outputs(h)
    back_even(jnp.logical_not(short))
    for g, t in turned:
        back_b(g, t)
    for g, t in turned:
        finish(g, t)

    for cond, sem, block in (
        (ahead, fs_sem.at[B], kv.at[:, :, own_rows]),
        (x_out, fs_sem.at[X], kv.at[:, :, own_rows]),
        (t_out, fs_sem.at[T], kv.at[:, :, own_rows]),
        (behind, bs_sem.at[B], kv.at[:, :, own_rows]),
        (x_in, bs_sem.at[X], kv.at[:, :, own_rows]),
        (t_in, bs_sem.at[T], kv.at[:, :, own_rows]),
    ):
        @pl.when(cond)
        def _():
            drain(sem, block)


def put_out(*refs):
    sems = refs[-1]
    copies = [
        pltpu.make_async_copy(refs[t], refs[4 + t], sems.at[t]) for t in range(4)
    ]
    for c in copies:
        c.start()
    for c in copies:
        c.wait()


def shards(doc_lengths, queries, key_states, value_head_states, out_grad):
    tok = queries.shape[0]
    heads = key_states.shape[1] // HEAD
    q_heads = queries.shape[1] // HEAD
    n = lax.axis_size("cp")
    window = (REACH + 1) * tok
    bf16, f32 = jnp.bfloat16, jnp.float32
    hbm_spec = pl.BlockSpec(memory_space=pltpu.HBM)
    any_spec = pl.BlockSpec(memory_space=pl.ANY)
    dma = pltpu.SemaphoreType.DMA
    args = [
        pltpu.with_memory_space_constraint(x, pltpu.HBM)
        for x in (doc_lengths, queries, key_states, value_head_states, out_grad)
    ]
    outs = pl.pallas_call(
        functools.partial(kernel, n, doc_lengths.shape[0]),
        out_shape=[
            jax.ShapeDtypeStruct(queries.shape, bf16),
            jax.ShapeDtypeStruct(queries.shape, bf16),
            jax.ShapeDtypeStruct(key_states.shape, bf16),
            jax.ShapeDtypeStruct(key_states.shape, bf16),
        ],
        in_specs=[hbm_spec] * 5,
        out_specs=[pl.BlockSpec(memory_space=pltpu.VMEM)] * 4,
        scratch_shapes=[
            pltpu.VMEM((heads, 2, window, HEAD), bf16),
            pltpu.VMEM((2, q_heads, tok, HEAD), bf16),
            pltpu.VMEM((heads, 2, tok, HEAD), f32),
            pltpu.VMEM((heads, 2, 2 * tok, HEAD), f32),
            pltpu.VMEM((heads, 2, REACH * tok, HEAD), bf16),
            pltpu.VMEM((3, heads, 2, tok, HEAD), bf16),
            pltpu.VMEM((heads, window, q_heads // heads * tok), bf16),
            pltpu.VMEM((heads, window, q_heads // heads * tok), bf16),
            pltpu.VMEM((window, tok), f32),
            pltpu.SMEM(doc_lengths.shape, jnp.int32),
            dma(()),
            dma((heads, 2)),
            dma((heads,)),
            dma((3,)),
            dma((3, heads, 2)),
            dma((3,)),
            dma((3, heads, 2)),
        ],
        compiler_params=pltpu.CompilerParams(
            collective_id=0, has_side_effects=True, vmem_limit_bytes=24 * 2**20),
        name="attend",
    )(*args)
    return tuple(pl.pallas_call(
        put_out,
        out_shape=[jax.ShapeDtypeStruct(x.shape, x.dtype) for x in outs],
        in_specs=[any_spec] * 4,
        out_specs=[hbm_spec] * 4,
        scratch_shapes=[dma((4,))],
        compiler_params=pltpu.CompilerParams(vmem_limit_bytes=2**20),
        name="put_out",
    )(*outs))


def solution(mesh):
    wide = P(("group", "cp"), "hd")
    return jax.shard_map(
        shards,
        mesh=mesh,
        in_specs=(P("group"), wide, wide, wide, wide),
        out_specs=(wide, wide, wide, wide),
        check_vma=False,
    )
```

```python
import functools
import math

import jax
import jax.numpy as jnp
from jax import lax
from jax.experimental import pallas as pl
from jax.experimental.pallas import tpu as pltpu
from jax.sharding import PartitionSpec as P

HEAD = 128
REACH = 3
MASKED = -1e30
MESH = pl.DeviceIdType.MESH
X, B, T = range(3)


def kernel(
    n, docs, doc_hbm, q_hbm, k_hbm, v_hbm, do_hbm, o_ref, gq_ref, gk_ref, gv_ref,
    kv, qd, own, mid, part, back, low_ref, grad_ref, bias, near, doc_ref,
    doc_sem, kv_sem, q_sem, fs_sem, fr_sem, bs_sem, br_sem,
):
    tok = q_hbm.shape[0]
    heads = k_hbm.shape[1] // HEAD
    group = q_hbm.shape[1] // k_hbm.shape[1]
    me = lax.axis_index("cp")
    odd = lax.rem(me, 2)
    is_odd = odd == 1
    is_even = odd == 0
    partner = me + 1 - 2 * odd
    short = lax.axis_index("hd") == 0
    own_rows = pl.ds(REACH * tok, tok)

    def rows(dist):
        return pl.ds((REACH - dist) * tok, tok)

    def cols(h):
        return pl.ds(h * HEAD, HEAD)

    doc_load = pltpu.make_async_copy(doc_hbm, doc_ref, doc_sem)
    doc_load.start()
    kv_loads = []
    for g in range(heads):
        kv_loads.append([
            pltpu.make_async_copy(src.at[:, cols(g)], kv.at[g, t, own_rows], kv_sem.at[g, t])
            for t, src in enumerate((k_hbm, v_hbm))
        ])
        for c in kv_loads[g]:
            c.start()
    for h in range(heads * group):
        for t, src in enumerate((q_hbm, do_hbm)):
            pltpu.make_async_copy(
                src.at[:, cols(h)], qd.at[t, h], q_sem.at[h // group]).start()

    barrier = pltpu.get_barrier_semaphore()
    for to, cond in ((me - 2, me >= 2), (me + 2, me + 2 < n), (partner, me >= 0)):
        @pl.when(cond)
        def _():
            pl.semaphore_signal(barrier, inc=1, device_id={"cp": to}, device_id_type=MESH)
    pl.semaphore_wait(
        barrier,
        1 + jnp.minimum(me // 2, 1) + jnp.minimum((n - 1 - me) // 2, 1))


    def fwd(kind, g, t, src_rows, dst_rows, to):
        return pltpu.make_async_remote_copy(
            src_ref=kv.at[g, t, src_rows], dst_ref=kv.at[g, t, dst_rows],
            send_sem=fs_sem.at[kind], recv_sem=fr_sem.at[kind, g, t],
            device_id={"cp": to}, device_id_type=MESH,
        )

    def drain(sem, block):
        pltpu.make_async_remote_copy(
            src_ref=block, dst_ref=block, send_sem=sem, recv_sem=fr_sem.at[X, 0, 0],
            device_id={"cp": partner}, device_id_type=MESH,
        ).wait_send()

    def fwd_x(g, t):
        return fwd(X, g, t, pl.ds((REACH - 2 * odd) * tok, tok), rows(1), partner)

    def fwd_b(g, t):
        return fwd(B, g, t, own_rows, rows(2), me + 2)

    def fwd_t(g, t):
        return fwd(T, g, t, rows(1), rows(3), me + 2)

    ahead = me + 2 < n
    behind = me >= 2
    x_in = is_odd | (me >= 2)
    x_out = is_even | (me >= 3)
    t_out = ahead & (me >= 1)
    t_in = me >= 3
    parts = [(g, t) for g in range(heads) for t in range(2)]
    turned = [(g, 1 - t) for g, t in parts]

    last = heads - 1
    early = 4

    def send_own(cond, g, t):
        @pl.when(cond & ahead)
        def _():
            fwd_b(g, t).start()
        @pl.when(cond & is_even)
        def _():
            fwd_x(g, t).start()

    for i, (g, t) in enumerate(parts):
        kv_loads[g][t].wait()
        send_own(short if i >= early else me >= 0, g, t)

    for dist in range(1, REACH + 1):
        @pl.when(me < dist)
        def _():
            kv[:, :, (REACH - dist) * tok:(REACH - dist + 1) * tok, :] = jnp.zeros(
                (heads, 2, tok, HEAD), kv.dtype)

    window = (REACH + 1) * tok
    key_pos = (me - REACH) * tok + lax.broadcasted_iota(jnp.int32, (window, tok), 0)
    query_pos = me * tok + lax.broadcasted_iota(jnp.int32, (window, tok), 1)

    doc_load.wait()
    end = jnp.int32(0)
    crossed = jnp.zeros((window, tok), jnp.int32)
    def count(d, carry):
        end, crossed = carry
        end = end + doc_ref[d]
        return end, crossed + jnp.where((key_pos < end) & (query_pos >= end), 1, 0)
    if docs <= 8:
        for d in range(docs):
            end, crossed = count(d, (end, crossed))
    else:
        end, crossed = lax.fori_loop(0, docs, count, (end, crossed))
    allowed = (crossed == 0) & (key_pos <= query_pos) & (key_pos >= 0)
    full = jnp.where(allowed, 0.0, MASKED)
    mine = (lax.broadcasted_iota(jnp.int32, (tok, tok), 0)
            <= lax.broadcasted_iota(jnp.int32, (tok, tok), 1))
    bias[:tok] = jnp.where(mine, full[REACH * tok:], full[:tok])
    bias[tok:] = full[tok:REACH * tok]
    near[...] = jnp.where(mine, 1.0, 0.0).astype(near.dtype)

    def relay_x(g, t):
        @pl.when(behind)
        def _():
            fwd_b(g, t).wait_recv()
        @pl.when(is_odd & (me >= 3))
        def _():
            fwd_x(g, t).start()

    def x_arrive(g, t):
        @pl.when(is_odd)
        def _():
            fwd_x(g, t).wait_recv()
        @pl.when(is_odd & ahead)
        def _():
            fwd_t(g, t).start()

    def relay_t(g, t, now):
        @pl.when(now & is_even & behind)
        def _():
            fwd_x(g, t).wait_recv()
        @pl.when(now & is_even & t_out)
        def _():
            fwd_t(g, t).start()

    def arrive(g):
        @pl.when(t_in)
        def _():
            for t in range(2):
                fwd_t(g, t).wait_recv()

    def bwd(kind, g, t, src_rows, to):
        return pltpu.make_async_remote_copy(
            src_ref=part.at[g, t, src_rows], dst_ref=back.at[kind, g, t],
            send_sem=bs_sem.at[kind], recv_sem=br_sem.at[kind, g, t],
            device_id={"cp": to}, device_id_type=MESH,
        )

    def bwd_x(g, t):
        return bwd(X, g, t, rows(1), partner)

    def bwd_b(g, t):
        return bwd(B, g, t, rows(2), me - 2)

    def bwd_t(g, t):
        return bwd(T, g, t, rows(3), me - 2)

    score_scale = 1.0 / math.sqrt(HEAD)
    exp_scale = score_scale * math.log2(math.e)
    nt = (((1,), (1,)), ((), ()))
    width = group * tok

    def cotangents(t, g):
        return qd[t, g * group:(g + 1) * group].reshape(width, HEAD)

    def compute(g):
        keys = kv[g, 0]
        values = kv[g, 1]
        mask = jnp.concatenate([bias[...]] * group, axis=1)
        near_low = jnp.concatenate([near[...]] * group, axis=1)
        nearer = jnp.concatenate([mine] * group, axis=1)

        def join(x):
            return jnp.concatenate(
                [jnp.where(nearer, x[REACH * tok:], x[:tok]), x[tok:REACH * tok]], axis=0)

        def split(x):
            own_part = x[:tok] * near_low
            return jnp.concatenate([x[:tok] - own_part, x[tok:], own_part], axis=0)

        loaded = qd.at[:, g * group:(g + 1) * group]
        pltpu.make_async_copy(loaded, loaded, q_sem.at[g]).wait()
        qs = cotangents(0, g)
        ds = cotangents(1, g)
        scores = join(lax.dot_general(keys, qs, nt, preferred_element_type=jnp.float32)) + mask
        top = jnp.max(scores, axis=0, keepdims=True)
        raw = jnp.exp2((scores - top) * exp_scale)
        probs = raw * (1.0 / jnp.sum(raw, axis=0, keepdims=True))
        low = split(probs.astype(jnp.bfloat16))
        low_ref[g] = low
        keep(g, 1, jnp.dot(low, ds, preferred_element_type=jnp.float32))
        back_start(g, 1)
        grad_p = join(lax.dot_general(values, ds, nt, preferred_element_type=jnp.float32))
        delta = jnp.sum(probs * grad_p, axis=0, keepdims=True)
        grad_s = split((probs * (grad_p - delta)).astype(jnp.bfloat16))
        grad_ref[g] = grad_s
        keep(g, 0, jnp.dot(grad_s, qs, preferred_element_type=jnp.float32) * score_scale)
        back_start(g, 0)

    def keep(g, t, grad):
        part[g, t] = grad[:REACH * tok].astype(part.dtype)
        mid[g, t] = grad[tok:REACH * tok]
        own[g, t] = grad[REACH * tok:]

    def outputs(g):
        for t, weights, out, scale in ((1, low_ref, o_ref, 1.0), (0, grad_ref, gq_ref, score_scale)):
            res = jnp.dot(kv[g, t].T, weights[g], preferred_element_type=jnp.float32) * scale
            for j in range(group):
                out[:, cols(g * group + j)] = (
                    res[:, j * tok:(j + 1) * tok].T.astype(out.dtype))

    def back_start(g, t):
        @pl.when(t_in)
        def _():
            bwd_t(g, t).start()

    def back_even(cond):
        @pl.when(is_even & behind & cond)
        def _():
            for g, t in turned:
                bwd_b(g, t).start()

    def back_x(g, t):
        @pl.when(t_out)
        def _():
            bwd_t(g, t).wait_recv()
            part[g, t, 2 * tok:] = (
                mid[g, t, tok:] + back[T, g, t].astype(jnp.float32)).astype(part.dtype)
        @pl.when(x_in)
        def _():
            bwd_x(g, t).start()

    def back_b(g, t):
        @pl.when(is_odd & (me >= 3))
        def _():
            bwd_x(g, t).wait_recv()
            part[g, t, tok:2 * tok] = (
                mid[g, t, :tok] + back[X, g, t].astype(jnp.float32)).astype(part.dtype)
            bwd_b(g, t).start()

    def finish(g, t):
        @pl.when(is_even)
        def _():
            bwd_x(g, t).wait_recv()
            own[g, t] = own[g, t] + back[X, g, t].astype(jnp.float32)
        @pl.when(ahead)
        def _():
            bwd_b(g, t).wait_recv()
            own[g, t] = own[g, t] + back[B, g, t].astype(jnp.float32)
        out = gv_ref if t else gk_ref
        out[:, cols(g)] = own[g, t].astype(out.dtype)

    for i, (g, t) in enumerate(parts):
        relay_x(g, t)
        if i + early < len(parts):
            send_own(jnp.logical_not(short), *parts[i + early])
        x_arrive(g, t)
    for g, t in parts[:-2]:
        relay_t(g, t, me >= 0)
    for g in range(heads):
        arrive(g)
        compute(g)
        for when, core in ((0, short), (min(1, last), jnp.logical_not(short))):
            if g == when:
                for t in range(2):
                    relay_t(last, t, core)
    back_even(short)
    for h in range(heads):
        for t in (1, 0):
            back_x(h, t)
        outputs(h)
    back_even(jnp.logical_not(short))
    for g, t in turned:
        back_b(g, t)
    for g, t in turned:
        finish(g, t)

    for cond, sem, block in (
        (ahead, fs_sem.at[B], kv.at[:, :, own_rows]),
        (x_out, fs_sem.at[X], kv.at[:, :, own_rows]),
        (t_out, fs_sem.at[T], kv.at[:, :, own_rows]),
        (behind, bs_sem.at[B], kv.at[:, :, own_rows]),
        (x_in, bs_sem.at[X], kv.at[:, :, own_rows]),
        (t_in, bs_sem.at[T], kv.at[:, :, own_rows]),
    ):
        @pl.when(cond)
        def _():
            drain(sem, block)


def put_out(*refs):
    sems = refs[-1]
    copies = [
        pltpu.make_async_copy(refs[t], refs[4 + t], sems.at[t]) for t in range(4)
    ]
    for c in copies:
        c.start()
    for c in copies:
        c.wait()


def shards(doc_lengths, queries, key_states, value_head_states, out_grad):
    tok = queries.shape[0]
    heads = key_states.shape[1] // HEAD
    q_heads = queries.shape[1] // HEAD
    n = lax.axis_size("cp")
    window = (REACH + 1) * tok
    bf16, f32 = jnp.bfloat16, jnp.float32
    hbm_spec = pl.BlockSpec(memory_space=pltpu.HBM)
    any_spec = pl.BlockSpec(memory_space=pl.ANY)
    dma = pltpu.SemaphoreType.DMA
    args = [
        pltpu.with_memory_space_constraint(x, pltpu.HBM)
        for x in (doc_lengths, queries, key_states, value_head_states, out_grad)
    ]
    outs = pl.pallas_call(
        functools.partial(kernel, n, doc_lengths.shape[0]),
        out_shape=[
            jax.ShapeDtypeStruct(queries.shape, bf16),
            jax.ShapeDtypeStruct(queries.shape, bf16),
            jax.ShapeDtypeStruct(key_states.shape, bf16),
            jax.ShapeDtypeStruct(key_states.shape, bf16),
        ],
        in_specs=[hbm_spec] * 5,
        out_specs=[pl.BlockSpec(memory_space=pltpu.VMEM)] * 4,
        scratch_shapes=[
            pltpu.VMEM((heads, 2, window, HEAD), bf16),
            pltpu.VMEM((2, q_heads, tok, HEAD), bf16),
            pltpu.VMEM((heads, 2, tok, HEAD), f32),
            pltpu.VMEM((heads, 2, 2 * tok, HEAD), f32),
            pltpu.VMEM((heads, 2, REACH * tok, HEAD), bf16),
            pltpu.VMEM((3, heads, 2, tok, HEAD), bf16),
            pltpu.VMEM((heads, window, q_heads // heads * tok), bf16),
            pltpu.VMEM((heads, window, q_heads // heads * tok), bf16),
            pltpu.VMEM((REACH * tok, tok), f32),
            pltpu.VMEM((tok, tok), bf16),
            pltpu.SMEM(doc_lengths.shape, jnp.int32),
            dma(()),
            dma((heads, 2)),
            dma((heads,)),
            dma((3,)),
            dma((3, heads, 2)),
            dma((3,)),
            dma((3, heads, 2)),
        ],
        compiler_params=pltpu.CompilerParams(
            collective_id=0, has_side_effects=True, vmem_limit_bytes=24 * 2**20),
        name="attend",
    )(*args)
    return tuple(pl.pallas_call(
        put_out,
        out_shape=[jax.ShapeDtypeStruct(x.shape, x.dtype) for x in outs],
        in_specs=[any_spec] * 4,
        out_specs=[hbm_spec] * 4,
        scratch_shapes=[dma((4,))],
        compiler_params=pltpu.CompilerParams(vmem_limit_bytes=2**20),
        name="put_out",
    )(*outs))


def solution(mesh):
    wide = P(("group", "cp"), "hd")
    return jax.shard_map(
        shards,
        mesh=mesh,
        in_specs=(P("group"), wide, wide, wide, wide),
        out_specs=(wide, wide, wide, wide),
        check_vma=False,
    )
```
